32 devices in a mesh: seq: 32 (over z, y, x, core).
Axes of the slice: x: 2, y: 2, z: 4, core: 2. Of those that a mesh axis runs over, the one named last changes fastest.
Arguments:
- queries: bfloat16 [16, 8192], P(None, 'seq'), may hold values from -1000 to 1000
- span_keys: bfloat16 [16, 1024], P(None, 'seq'), may hold values from -6 to 6
- span_values: bfloat16 [16, 1024], P(None, 'seq'), may hold values from -6 to 6
- positions: int32 [3, 16], replicated, may hold values from 0 to 8191, as said below
- span_segments: int32 [16], replicated, may hold values from 0 to 3, as said below
- cache_keys: bfloat16 [16384, 1024], P('seq'), may hold values from -6 to 6
- cache_values: bfloat16 [16384, 1024], P('seq'), may hold values from -6 to 6
- cache_segments: int32 [16384], P('seq'), may hold values from 0 to 3
Outputs:
- attended: bfloat16 [16, 8192], replicated
The draws below stay inside these ranges and needn't reach their ends.
Inputs may be any that keep to these rules, and one draw needn't show every extreme that they name: `positions`: row 0 holds time ids; rows 1 and 2 hold height and width ids, which are below 64. `span_segments`: never falling; every request 0 to 3 has one run of rows, and every run starts at an even row.
All inputs are finite; a program needn't handle non-finite values.
Results may differ from the reference program's by a relative error of at most 0.0054.
Values may be sent and summed in bfloat16 or wider, within the bound.
A program may use at most 64 MiB of HBM per device.

```python
import jax
import jax.numpy as jnp
from jax import lax

H = 64
KVH = 8
HD = 128
REQS = 4
QROWS = 16
KV_DEV = 512
TOKENS = 16384
N_SEQ = 32


def position_table(key):
    base = jax.random.fold_in(key, 23)
    first, second = jax.random.split(base)
    times = jax.random.randint(first, (1, QROWS), 0, 8192)
    places = jax.random.randint(second, (2, QROWS), 0, 64)
    return jnp.concatenate([times, places], axis=0).astype(jnp.int32)


def span_segment_table(key):
    base = jax.random.fold_in(key, 37)
    order = jax.random.permutation(base, QROWS // 2 - 1) + 1
    starts = 2 * order[:REQS - 1]
    rows = jnp.arange(QROWS, dtype=jnp.int32)
    return jnp.sum((rows[:, None] >= starts[None, :]).astype(jnp.int32), axis=1).astype(jnp.int32)


def cache_segment_table(key):
    base = jax.random.fold_in(key, 53)
    return jax.random.randint(base, (TOKENS,), 0, REQS).astype(jnp.int32)


def span_pair(key):
    base = jax.random.fold_in(key, 11)
    parts = jax.random.split(base, 3)
    group = H // KVH
    keys = jnp.clip(jax.random.normal(parts[0], (QROWS, KVH, HD), jnp.float32), -6.0, 6.0)
    noise = jnp.clip(jax.random.normal(parts[1], (QROWS, KVH, group, HD), jnp.float32), -6.0, 6.0)
    pull = jax.random.uniform(parts[2], (QROWS, KVH, group, 1), jnp.float32, 0.9, 1.6)
    queries = 3.0 * noise + pull * keys[:, :, None, :]
    queries = jnp.clip(queries, -1000.0, 1000.0)
    keys = jnp.clip(keys, -6.0, 6.0)
    return (queries.reshape(QROWS, H * HD), keys.reshape(QROWS, KVH * HD))


def draw_queries(key, part):
    return span_pair(key)[0].astype(jnp.bfloat16)


def draw_span_keys(key, part):
    return span_pair(key)[1].astype(jnp.bfloat16)


def draw_positions(key, part):
    return position_table(key)


def draw_span_segments(key, part):
    return span_segment_table(key)


def draw_cache_segments(key, part):
    return cache_segment_table(key)


def draw_cache_keys(key, part):
    base = jax.random.fold_in(key, 71)
    parts = jax.random.split(base, 1)
    cache = jnp.clip(jax.random.normal(parts[0], (TOKENS, KVH, HD), jnp.float32), -6.0, 6.0)
    return jnp.clip(cache, -6.0, 6.0).reshape(TOKENS, KVH * HD).astype(jnp.bfloat16)


def level_of(own_key, extent, cuts, least, largest):
    gain, own = 1.0, jax.random.fold_in(own_key, 6)
    for dim, blocks in cuts:
        steps = jnp.exp(jax.random.uniform(jax.random.fold_in(own, dim), (blocks,), jnp.float32, least / len(cuts), largest / len(cuts)))
        gain = gain * jnp.repeat(steps, extent[dim] // blocks).reshape([-1 if axis == dim else 1 for axis in range(len(extent))])
    return gain


def centred(key, shape, spread, reach, cuts=(), held_as=jnp.bfloat16):
    entries = spread * jax.random.normal(key, shape, jnp.float32)
    if cuts:
        entries = entries * level_of(key, shape, cuts, -0.22, 0.18)
    return jnp.clip(entries, -reach, reach).astype(held_as)


def setup_inputs(seed: int = 0) -> dict:
    streams_of = jax.random.split(jax.random.key(seed), 9)
    return {
        "queries": draw_queries(jax.random.fold_in(streams_of[8], 71), 0),
        "span_keys": draw_span_keys(jax.random.fold_in(streams_of[8], 71), 0),
        "span_values": centred(streams_of[2], (QROWS, KVH * HD), 1.0, 6.0, ((1, 32),)),
        "positions": draw_positions(jax.random.fold_in(streams_of[8], 71), 0),
        "span_segments": draw_span_segments(jax.random.fold_in(streams_of[8], 71), 0),
        "cache_keys": draw_cache_keys(jax.random.fold_in(streams_of[8], 71), 0),
        "cache_values": centred(streams_of[6], (TOKENS, KVH * HD), 1.0, 6.0, ((0, 32),)),
        "cache_segments": draw_cache_segments(jax.random.fold_in(streams_of[8], 71), 0),
    }


def rope_tables(positions, head_dim):
    half = head_dim // 2
    index = jnp.arange(half, dtype=jnp.int32)
    inverse = jnp.power(jnp.float32(1000000.0), -2.0 * index.astype(jnp.float32) / head_dim)
    section = jnp.where(index < head_dim // 8, 0, jnp.where(index < 5 * head_dim // 16, 1, 2))
    chosen = jnp.where(section[None, :] == 0, positions[0][:, None],
                       jnp.where(section[None, :] == 1, positions[1][:, None], positions[2][:, None]))
    angle = chosen.astype(jnp.float32) * inverse[None, :]
    return jnp.cos(angle), jnp.sin(angle)


def rotate(values, cosines, sines):
    half = values.shape[-1] // 2
    first = values[..., :half]
    second = values[..., half:]
    cosine = cosines[:, None, :]
    sine = sines[:, None, :]
    return jnp.concatenate([first * cosine - second * sine, second * cosine + first * sine], axis=-1)


def head_state(q_rot, keys, values, visible):
    rows, kv_heads, group, head_dim = q_rot.shape
    scale = 1.0 / (head_dim ** 0.5)
    outs, peaks, totals = [], [], []
    for head in range(kv_heads):
        block = q_rot[:, head].reshape(rows * group, head_dim)
        key_cols = keys[:, head * head_dim:(head + 1) * head_dim]
        value_cols = values[:, head * head_dim:(head + 1) * head_dim]
        scores = lax.dot_general(block, key_cols, (((1,), (1,)), ((), ())),
                                 preferred_element_type=jnp.float32) * scale
        scores = scores.reshape(rows, group, -1)
        mask = visible[:, None, :]
        peak = jnp.max(jnp.where(mask, scores, jnp.float32(-1e30)), axis=-1)
        weights = jnp.where(mask, jnp.exp(scores - peak[..., None]), jnp.float32(0.0))
        total = jnp.sum(weights, axis=-1)
        out = jnp.dot(weights.astype(jnp.bfloat16).reshape(rows * group, -1), value_cols,
                      preferred_element_type=jnp.float32)
        outs.append(out.reshape(rows, group, head_dim))
        peaks.append(peak)
        totals.append(total)
    out_all = jnp.stack(outs, axis=1).reshape(rows * kv_heads * group, head_dim)
    peak_all = jnp.stack(peaks, axis=1).reshape(rows * kv_heads * group)
    total_all = jnp.stack(totals, axis=1).reshape(rows * kv_heads * group)
    return out_all, peak_all, total_all


def combine(left, right):
    out_a, peak_a, total_a = left
    out_b, peak_b, total_b = right
    peak = jnp.maximum(peak_a, peak_b)
    factor_a = jnp.exp(peak_a - peak)
    factor_b = jnp.exp(peak_b - peak)
    return (out_a * factor_a[:, None] + out_b * factor_b[:, None], peak,
            total_a * factor_a + total_b * factor_b)


def reference(queries, span_keys, span_values, positions, span_segments, cache_keys, cache_values, cache_segments):
    group = H // KVH
    cosines, sines = rope_tables(positions, HD)
    q_rot = rotate(queries.astype(jnp.float32).reshape(QROWS, H, HD), cosines, sines).astype(jnp.bfloat16)
    q_rot = q_rot.reshape(QROWS, KVH, group, HD)
    k_rot = rotate(span_keys.astype(jnp.float32).reshape(QROWS, KVH, HD), cosines, sines)
    k_rot = k_rot.astype(jnp.bfloat16).reshape(QROWS, KVH * HD)
    index = jnp.arange(QROWS, dtype=jnp.int32)
    own_visible = (span_segments[:, None] == span_segments[None, :]) & (index[None, :] <= index[:, None])
    span_state = head_state(q_rot, k_rot, span_values, own_visible)

    key_blocks = cache_keys.reshape(N_SEQ, KV_DEV, KVH * HD)
    value_blocks = cache_values.reshape(N_SEQ, KV_DEV, KVH * HD)
    segment_blocks = cache_segments.reshape(N_SEQ, KV_DEV)

    def step(carry, block):
        keys, values, segments = block
        visible = span_segments[:, None] == segments[None, :]
        return combine(carry, head_state(q_rot, keys, values, visible)), None

    start = (jnp.zeros((QROWS * H, HD), jnp.float32), jnp.full((QROWS * H,), -1e30, jnp.float32),
             jnp.zeros((QROWS * H,), jnp.float32))
    cache_state, _ = lax.scan(step, start, (key_blocks, value_blocks, segment_blocks))
    merged_out, _, merged_total = combine(cache_state, span_state)
    return (merged_out / merged_total[:, None]).astype(jnp.bfloat16).reshape(QROWS, H * HD)
```

```python
import functools
import math

import jax
import jax.numpy as jnp
import numpy as np
from jax import lax
from jax.experimental import pallas as pl
from jax.experimental.pallas import tpu as pltpu
from jax.sharding import PartitionSpec as P

H = 64
KVH = 8
HD = 128
MESH = pl.DeviceIdType.MESH
HIDDEN = -1e30
FLOOR = -1e29


def rope_tables(pos, rows):
    half = HD // 2
    lane = lax.broadcasted_iota(jnp.int32, (rows, HD), 1)
    row = lax.broadcasted_iota(jnp.int32, (rows, HD), 0)
    index = lax.rem(lane, half)
    inverse = jnp.zeros((rows, HD), jnp.float32)
    for j in range(half):
        inverse = jnp.where(index == j, jnp.float32(np.float32(1e6 ** (-2.0 * j / HD))), inverse)
    chosen = []
    for c in range(3):
        spread = jnp.zeros((rows, HD), jnp.int32)
        for r in range(rows):
            spread = jnp.where(row == r, pos[c, r], spread)
        chosen.append(spread)
    picked = jnp.where(
        index < HD // 8, chosen[0], jnp.where(index < 5 * HD // 16, chosen[1], chosen[2])
    )
    angle = picked.astype(jnp.float32) * inverse
    sine = jnp.sin(angle)
    return jnp.cos(angle), jnp.where(lane < half, -sine, sine)


def columns(buf, start, width):
    if width >= HD:
        slot, off = start // width, start % width
        return buf[slot, :, off : off + HD].astype(jnp.float32)
    first = start // width
    return jnp.concatenate(
        [buf[first + i].astype(jnp.float32) for i in range(HD // width)], axis=1
    )


def kernel(
    n,
    q_hbm,
    k_hbm,
    v_hbm,
    pos_hbm,
    seg_hbm,
    ck_hbm,
    cv_hbm,
    cs_hbm,
    out_ref,
    q_own,
    k_own,
    v_own,
    pos,
    seg,
    keys,
    values,
    cseg,
    q_all,
    k_all,
    v_all,
    k_span,
    v_span,
    values_t,
    bias,
    part_out,
    part_ml,
    got_out,
    got_ml,
    piece,
    pieces,
    load_sem,
    q_sem,
    kv_sem,
    part_sem,
    ml_sem,
    piece_sem,
    send_sem,
):
    me = lax.axis_index("seq")
    rows, width = q_own.shape
    kwidth = k_own.shape[1]
    tokens = keys.shape[0]
    per = n // KVH
    share = HD // per
    mine = me // per

    loads = [
        pltpu.make_async_copy(src, dst, load_sem.at[i])
        for i, (src, dst) in enumerate(
            (
                (q_hbm, q_own),
                (k_hbm, k_own),
                (v_hbm, v_own),
                (pos_hbm, pos),
                (seg_hbm, seg),
                (cs_hbm, cseg),
                (cv_hbm, values),
                (ck_hbm, keys),
            )
        )
    ]
    for load in loads:
        load.start()

    barrier = pltpu.get_barrier_semaphore()

    @pl.loop(1, n)
    def _(i):
        pl.semaphore_signal(
            barrier, inc=1, device_id=(lax.rem(me + i, n),), device_id_type=MESH
        )

    for load in loads[:3]:
        load.wait()
    own_q = pltpu.make_async_copy(q_own, q_all.at[me], q_sem.at[mine])
    own_q.start()
    pl.semaphore_wait(barrier, n - 1)

    @pl.loop(1, n)
    def _(i):
        pltpu.make_async_remote_copy(
            src_ref=q_own,
            dst_ref=q_all.at[me],
            send_sem=send_sem.at[0],
            recv_sem=q_sem.at[mine],
            device_id=(lax.rem(me + i, n),),
            device_id_type=MESH,
        ).start()

    @pl.when(me != 0)
    def _():
        for i, (src, dst) in enumerate(((k_own, k_all), (v_own, v_all))):
            pltpu.make_async_remote_copy(
                src_ref=src,
                dst_ref=dst.at[me],
                send_sem=send_sem.at[1 + i],
                recv_sem=kv_sem.at[i],
                device_id=(0,),
                device_id_type=MESH,
            ).start()

    @pl.when(me == 0)
    def _():
        for i, (src, dst) in enumerate(((k_own, k_all), (v_own, v_all))):
            pltpu.make_async_copy(src, dst.at[me], kv_sem.at[i]).start()

    for load in loads[3:]:
        load.wait()
    cosine, sine = rope_tables(pos, rows)
    lane = lax.broadcasted_iota(jnp.int32, (1, HD), 1)
    lane_row = lax.rem(lane, rows)
    lane_seg = jnp.zeros((1, HD), jnp.int32)
    for r in range(rows):
        lane_seg = jnp.where(lane_row == r, seg[r], lane_seg)
    lane_seg = lane_seg.astype(jnp.float32)
    for c in range(tokens // HD):
        across = cseg[:, c * HD : (c + 1) * HD].astype(jnp.float32)
        down = jnp.transpose(jnp.broadcast_to(across, (HD, HD)))
        bias[c * HD : (c + 1) * HD, :] = jnp.where(down == lane_seg, 0.0, HIDDEN)
    token = lax.broadcasted_iota(jnp.int32, (rows, HD), 0)
    token_seg = jnp.zeros((rows, HD), jnp.int32)
    for r in range(rows):
        token_seg = jnp.where(token == r, seg[r], token_seg)
    seen = (token_seg.astype(jnp.float32) == lane_seg) & (token <= lane_row)
    holder = jnp.where(me == 0, 0.0, HIDDEN)
    span_bias = jnp.where(seen, holder, HIDDEN)
    for g in range(KVH):
        values_t[g] = jnp.transpose(values[:, g * HD : (g + 1) * HD])

    @pl.when(me == 0)
    def _():
        for i, dst in enumerate((k_all, v_all)):
            pltpu.make_async_copy(dst, dst, kv_sem.at[i]).wait()
        for g in range(KVH):
            cols = slice(g * HD, (g + 1) * HD)
            k = columns(k_all, g * HD, kwidth)
            k_span[:, cols] = (k * cosine + pltpu.roll(k, HD // 2, 1) * sine).astype(jnp.bfloat16)
            v_span[:, cols] = columns(v_all, g * HD, kwidth).astype(jnp.bfloat16)

    @pl.when(me != 0)
    def _():
        k_span[...] = jnp.zeros_like(k_span)
        v_span[...] = jnp.zeros_like(v_span)

    contract_last = (((1,), (1,)), ((), ()))
    contract_first = (((0,), (0,)), ((), ()))
    factor = math.log2(math.e) / math.sqrt(HD)
    group = H // KVH
    for g in range(KVH):
        cols = slice(g * HD, (g + 1) * HD)
        landed = q_all.at[pl.ds(g * per, per)]
        pltpu.make_async_copy(landed, landed, q_sem.at[g]).wait()
        heads = []
        for i in range(group):
            q = columns(q_all, (g * group + i) * HD, width)
            heads.append((q * cosine + pltpu.roll(q, HD // 2, 1) * sine).astype(jnp.bfloat16))
        block = jnp.concatenate(heads, axis=0)
        scores = (
            lax.dot_general(keys[:, cols], block, contract_last, preferred_element_type=jnp.float32)
            + bias[...]
        )
        span_scores = (
            lax.dot_general(
                k_span[:, cols], block, contract_last, preferred_element_type=jnp.float32
            )
            + span_bias
        )
        peak = jnp.maximum(
            jnp.max(scores, axis=0, keepdims=True), jnp.max(span_scores, axis=0, keepdims=True)
        )
        peak = jnp.maximum(peak, FLOOR)
        weights = jnp.exp2((scores - peak) * factor)
        span_weights = jnp.exp2((span_scores - peak) * factor)
        total = jnp.sum(weights, axis=0, keepdims=True) + jnp.sum(
            span_weights, axis=0, keepdims=True
        )
        out = jnp.dot(
            values_t[g], weights.astype(jnp.bfloat16), preferred_element_type=jnp.float32
        ) + lax.dot_general(
            v_span[:, cols],
            span_weights.astype(jnp.bfloat16),
            contract_first,
            preferred_element_type=jnp.float32,
        )
        part_ml[g, 0:1, :] = peak
        part_ml[g, 1:2, :] = total
        for j in range(per):
            part_out[g * per + j] = out[j * share : (j + 1) * share].astype(jnp.bfloat16)

        @pl.loop(0, per)
        def _(j):
            dest = g * per + j

            @pl.when(dest != me)
            def _():
                pltpu.make_async_remote_copy(
                    src_ref=part_out.at[dest],
                    dst_ref=got_out.at[me],
                    send_sem=send_sem.at[3],
                    recv_sem=part_sem,
                    device_id=(dest,),
                    device_id_type=MESH,
                ).start()
                pltpu.make_async_remote_copy(
                    src_ref=part_ml.at[g],
                    dst_ref=got_ml.at[me],
                    send_sem=send_sem.at[4],
                    recv_sem=ml_sem,
                    device_id=(dest,),
                    device_id_type=MESH,
                ).start()

            @pl.when(dest == me)
            def _():
                pltpu.make_async_copy(part_out.at[dest], got_out.at[me], part_sem).start()
                pltpu.make_async_copy(part_ml.at[g], got_ml.at[me], ml_sem).start()

    pltpu.make_async_copy(got_ml, got_ml, ml_sem).wait()
    peaks = got_ml[:, 0, :]
    scale = jnp.exp2((peaks - jnp.max(peaks, axis=0, keepdims=True)) * factor)
    whole = jnp.sum(scale * got_ml[:, 1, :], axis=0, keepdims=True)
    scale = scale / whole
    pltpu.make_async_copy(got_out, got_out, part_sem).wait()
    merged = jnp.zeros((share, HD), jnp.float32)
    for s in range(n):
        merged = merged + got_out[s].astype(jnp.float32) * scale[s : s + 1, :]
    piece[...] = merged.astype(jnp.bfloat16)

    @pl.loop(1, n)
    def _(i):
        pltpu.make_async_remote_copy(
            src_ref=piece,
            dst_ref=pieces.at[me],
            send_sem=send_sem.at[5],
            recv_sem=piece_sem.at[mine],
            device_id=(lax.rem(me + i, n),),
            device_id_type=MESH,
        ).start()

    pltpu.make_async_copy(piece, pieces.at[me], piece_sem.at[mine]).start()

    for g in range(KVH):
        landed = pieces.at[pl.ds(g * per, per)]
        pltpu.make_async_copy(landed, landed, piece_sem.at[g]).wait()
        tall = jnp.concatenate(
            [pieces[g * per + j].astype(jnp.float32) for j in range(per)], axis=0
        )
        flat = jnp.transpose(tall).astype(jnp.bfloat16)
        for i in range(group):
            h = g * group + i
            out_ref[:, h * HD : (h + 1) * HD] = flat[i * rows : (i + 1) * rows]

    others = pl.ds(0, n - 1)
    for i, ref in ((0, q_all), (3, got_out), (4, got_ml), (5, pieces)):
        pltpu.make_async_copy(ref.at[others], ref.at[others], send_sem.at[i]).wait()

    @pl.when(me != 0)
    def _():
        pltpu.make_async_copy(k_own, k_own, send_sem.at[1]).wait()
        pltpu.make_async_copy(v_own, v_own, send_sem.at[2]).wait()


def solution(mesh):
    n = mesh.shape["seq"]

    def per_device(q, k, v, positions, span_segments, cache_keys, cache_values, cache_segments):
        rows, width = q.shape
        kwidth = k.shape[1]
        tokens = cache_keys.shape[0]
        share = KVH * HD // n
        bf16, f32, i32 = jnp.bfloat16, jnp.float32, jnp.int32
        return pl.pallas_call(
            functools.partial(kernel, n),
            out_shape=jax.ShapeDtypeStruct((rows, H * HD), bf16),
            in_specs=[pl.BlockSpec(memory_space=pl.ANY)] * 8,
            out_specs=pl.BlockSpec(memory_space=pltpu.VMEM),
            scratch_shapes=[
                pltpu.VMEM((rows, width), bf16),
                pltpu.VMEM((rows, kwidth), bf16),
                pltpu.VMEM((rows, kwidth), bf16),
                pltpu.SMEM(positions.shape, i32),
                pltpu.SMEM(span_segments.shape, i32),
                pltpu.VMEM((tokens, KVH * HD), bf16),
                pltpu.VMEM((tokens, KVH * HD), bf16),
                pltpu.VMEM((1, tokens), i32),
                pltpu.VMEM((n, rows, width), bf16),
                pltpu.VMEM((n, rows, kwidth), bf16),
                pltpu.VMEM((n, rows, kwidth), bf16),
                pltpu.VMEM((rows, KVH * HD), bf16),
                pltpu.VMEM((rows, KVH * HD), bf16),
                pltpu.VMEM((KVH, HD, tokens), bf16),
                pltpu.VMEM((tokens, HD), f32),
                pltpu.VMEM((n, share, HD), bf16),
                pltpu.VMEM((KVH, 2, HD), f32),
                pltpu.VMEM((n, share, HD), bf16),
                pltpu.VMEM((n, 2, HD), f32),
                pltpu.VMEM((share, HD), bf16),
                pltpu.VMEM((n, share, HD), bf16),
                pltpu.SemaphoreType.DMA((8,)),
                pltpu.SemaphoreType.DMA((KVH,)),
                pltpu.SemaphoreType.DMA((2,)),
                pltpu.SemaphoreType.DMA,
                pltpu.SemaphoreType.DMA,
                pltpu.SemaphoreType.DMA((KVH,)),
                pltpu.SemaphoreType.DMA((6,)),
            ],
            compiler_params=pltpu.CompilerParams(collective_id=0, has_side_effects=True),
        )(
            q,
            k,
            v,
            positions,
            span_segments,
            cache_keys,
            cache_values,
            cache_segments.reshape(1, tokens),
        )

    in_specs = (
        P(None, "seq"),
        P(None, "seq"),
        P(None, "seq"),
        P(),
        P(),
        P("seq", None),
        P("seq", None),
        P("seq"),
    )
    return jax.shard_map(
        per_device, mesh=mesh, in_specs=in_specs, out_specs=P(), check_vma=False
    )
```

```python
import functools
import math

import jax
import jax.numpy as jnp
import numpy as np
from jax import lax
from jax.experimental import pallas as pl
from jax.experimental.pallas import tpu as pltpu
from jax.sharding import PartitionSpec as P

H = 64
KVH = 8
HD = 128
MESH = pl.DeviceIdType.MESH
HIDDEN = -1e30
FLOOR = -1e29


def rope_tables(pos, rows):
    half = HD // 2
    lane = lax.broadcasted_iota(jnp.int32, (rows, HD), 1)
    row = lax.broadcasted_iota(jnp.int32, (rows, HD), 0)
    index = lax.rem(lane, half)
    inverse = jnp.zeros((rows, HD), jnp.float32)
    for j in range(half):
        inverse = jnp.where(index == j, jnp.float32(np.float32(1e6 ** (-2.0 * j / HD))), inverse)
    chosen = []
    for c in range(3):
        spread = jnp.zeros((rows, HD), jnp.int32)
        for r in range(rows):
            spread = jnp.where(row == r, pos[c, r], spread)
        chosen.append(spread)
    picked = jnp.where(
        index < HD // 8, chosen[0], jnp.where(index < 5 * HD // 16, chosen[1], chosen[2])
    )
    angle = picked.astype(jnp.float32) * inverse
    sine = jnp.sin(angle)
    return jnp.cos(angle), jnp.where(lane < half, -sine, sine)


def columns(buf, start, width):
    if width >= HD:
        slot, off = start // width, start % width
        return buf[slot, :, off : off + HD].astype(jnp.float32)
    first = start // width
    return jnp.concatenate(
        [buf[first + i].astype(jnp.float32) for i in range(HD // width)], axis=1
    )


def group_head(buf, g, head):
    width = buf.shape[3]
    base = g * (buf.shape[1] // KVH)
    if width >= HD:
        block, off = head * HD // width, head * HD % width
        return buf[block % 2, base + block // 2, :, off : off + HD].astype(jnp.float32)
    first = head * (HD // width)
    return jnp.concatenate(
        [
            buf[block % 2, base + block // 2].astype(jnp.float32)
            for block in range(first, first + HD // width)
        ],
        axis=1,
    )


def kernel(
    n,
    q_hbm,
    k_hbm,
    v_hbm,
    pos_hbm,
    seg_hbm,
    ck_hbm,
    cv_hbm,
    cs_hbm,
    out_ref,
    q_own,
    k_own,
    v_own,
    pos,
    seg,
    keys,
    values,
    cseg,
    q_all,
    k_all,
    v_all,
    k_span,
    v_span,
    values_t,
    bias,
    part_out,
    part_ml,
    got_out,
    got_ml,
    piece,
    pieces,
    load_sem,
    q_sem,
    q_pair_sem,
    kv_sem,
    part_sem,
    ml_sem,
    piece_sem,
    piece_pair_sem,
    send_sem,
):
    me = lax.axis_index("seq")
    rows, width = q_own.shape
    kwidth = k_own.shape[1]
    tokens = keys.shape[0]
    per = n // KVH
    share = HD // per
    mine = me // per
    half = per // 2
    core, chip = lax.rem(me, 2), me // 2
    pair = me + 1 - 2 * core

    def hand_on(buf, g, sem, pair_sem, sent):
        landed = buf.at[core, pl.ds(g * half, half)]
        pltpu.make_async_copy(landed, landed, sem.at[g]).wait()
        pltpu.make_async_remote_copy(
            src_ref=landed,
            dst_ref=landed,
            send_sem=sent,
            recv_sem=pair_sem.at[g],
            device_id=(pair,),
            device_id_type=MESH,
        ).start()

    def await_pair(buf, g, pair_sem):
        landed = buf.at[1 - core, pl.ds(g * half, half)]
        pltpu.make_async_copy(landed, landed, pair_sem.at[g]).wait()

    order = [lax.rem(mine + t, KVH) for t in range(KVH)]

    loads = [
        pltpu.make_async_copy(src, dst, load_sem.at[i])
        for i, (src, dst) in enumerate(
            (
                (q_hbm, q_own),
                (k_hbm, k_own),
                (v_hbm, v_own),
                (pos_hbm, pos),
                (seg_hbm, seg),
                (cs_hbm, cseg),
                (cv_hbm, values),
                (ck_hbm, keys),
            )
        )
    ]
    for load in loads:
        load.start()

    barrier = pltpu.get_barrier_semaphore()

    @pl.loop(1, n)
    def _(i):
        pl.semaphore_signal(
            barrier, inc=1, device_id=(lax.rem(me + i, n),), device_id_type=MESH
        )

    for load in loads[:3]:
        load.wait()
    own_q = pltpu.make_async_copy(q_own, q_all.at[core, chip], q_sem.at[mine])
    own_q.start()
    pl.semaphore_wait(barrier, n - 1)

    @pl.when(me != 0)
    def _():
        for i, (src, dst) in enumerate(((k_own, k_all), (v_own, v_all))):
            pltpu.make_async_remote_copy(
                src_ref=src,
                dst_ref=dst.at[me],
                send_sem=send_sem.at[1 + i],
                recv_sem=kv_sem.at[i],
                device_id=(0,),
                device_id_type=MESH,
            ).start()

    @pl.when(me == 0)
    def _():
        for i, (src, dst) in enumerate(((k_own, k_all), (v_own, v_all))):
            pltpu.make_async_copy(src, dst.at[me], kv_sem.at[i]).start()

    @pl.loop(1, n // 2)
    def _(i):
        pltpu.make_async_remote_copy(
            src_ref=q_own,
            dst_ref=q_all.at[core, chip],
            send_sem=send_sem.at[0],
            recv_sem=q_sem.at[mine],
            device_id=(lax.rem(me + 2 * i, n),),
            device_id_type=MESH,
        ).start()

    for load in loads[3:]:
        load.wait()
    cosine, sine = rope_tables(pos, rows)
    lane = lax.broadcasted_iota(jnp.int32, (1, HD), 1)
    lane_row = lax.rem(lane, rows)
    lane_seg = jnp.zeros((1, HD), jnp.int32)
    for r in range(rows):
        lane_seg = jnp.where(lane_row == r, seg[r], lane_seg)
    lane_seg = lane_seg.astype(jnp.float32)
    for c in range(tokens // HD):
        across = cseg[:, c * HD : (c + 1) * HD].astype(jnp.float32)
        down = jnp.transpose(jnp.broadcast_to(across, (HD, HD)))
        bias[c * HD : (c + 1) * HD, :] = jnp.where(down == lane_seg, 0.0, HIDDEN)
    token = lax.broadcasted_iota(jnp.int32, (rows, HD), 0)
    token_seg = jnp.zeros((rows, HD), jnp.int32)
    for r in range(rows):
        token_seg = jnp.where(token == r, seg[r], token_seg)
    seen = (token_seg.astype(jnp.float32) == lane_seg) & (token <= lane_row)
    holder = jnp.where(me == 0, 0.0, HIDDEN)
    span_bias = jnp.where(seen, holder, HIDDEN)
    for g in range(KVH):
        values_t[g] = jnp.transpose(values[:, g * HD : (g + 1) * HD])

    @pl.when(me == 0)
    def _():
        for i, dst in enumerate((k_all, v_all)):
            pltpu.make_async_copy(dst, dst, kv_sem.at[i]).wait()
        for g in range(KVH):
            cols = slice(g * HD, (g + 1) * HD)
            k = columns(k_all, g * HD, kwidth)
            k_span[:, cols] = (k * cosine + pltpu.roll(k, HD // 2, 1) * sine).astype(jnp.bfloat16)
            v_span[:, cols] = columns(v_all, g * HD, kwidth).astype(jnp.bfloat16)

    @pl.when(me != 0)
    def _():
        k_span[...] = jnp.zeros_like(k_span)
        v_span[...] = jnp.zeros_like(v_span)

    contract_last = (((1,), (1,)), ((), ()))
    contract_first = (((0,), (0,)), ((), ()))
    factor = math.log2(math.e) / math.sqrt(HD)
    group = H // KVH
    hand_on(q_all, order[0], q_sem, q_pair_sem, send_sem.at[6])
    for t, g in enumerate(order):
        cols = pl.ds(pl.multiple_of(g * HD, HD), HD)
        if t + 1 < KVH:
            hand_on(q_all, order[t + 1], q_sem, q_pair_sem, send_sem.at[6])
        await_pair(q_all, g, q_pair_sem)
        heads = []
        for i in range(group):
            q = group_head(q_all, g, i)
            heads.append((q * cosine + pltpu.roll(q, HD // 2, 1) * sine).astype(jnp.bfloat16))
        block = jnp.concatenate(heads, axis=0)
        scores = (
            lax.dot_general(keys[:, cols], block, contract_last, preferred_element_type=jnp.float32)
            + bias[...]
        )
        span_scores = (
            lax.dot_general(
                k_span[:, cols], block, contract_last, preferred_element_type=jnp.float32
            )
            + span_bias
        )
        peak = jnp.maximum(
            jnp.max(scores, axis=0, keepdims=True), jnp.max(span_scores, axis=0, keepdims=True)
        )
        peak = jnp.maximum(peak, FLOOR)
        weights = jnp.exp2((scores - peak) * factor)
        span_weights = jnp.exp2((span_scores - peak) * factor)
        total = jnp.sum(weights, axis=0, keepdims=True) + jnp.sum(
            span_weights, axis=0, keepdims=True
        )
        out = jnp.dot(
            values_t[g], weights.astype(jnp.bfloat16), preferred_element_type=jnp.float32
        ) + lax.dot_general(
            v_span[:, cols],
            span_weights.astype(jnp.bfloat16),
            contract_first,
            preferred_element_type=jnp.float32,
        )
        part_ml[g] = jnp.concatenate([peak, total], axis=0)
        for j in range(per):
            part_out[g * per + j] = out[j * share : (j + 1) * share].astype(jnp.bfloat16)

        @pl.loop(0, per)
        def _(j):
            dest = g * per + j

            @pl.when(dest != me)
            def _():
                pltpu.make_async_remote_copy(
                    src_ref=part_out.at[dest],
                    dst_ref=got_out.at[me],
                    send_sem=send_sem.at[3],
                    recv_sem=part_sem,
                    device_id=(dest,),
                    device_id_type=MESH,
                ).start()
                pltpu.make_async_remote_copy(
                    src_ref=part_ml.at[g],
                    dst_ref=got_ml.at[me],
                    send_sem=send_sem.at[4],
                    recv_sem=ml_sem,
                    device_id=(dest,),
                    device_id_type=MESH,
                ).start()

            @pl.when(dest == me)
            def _():
                pltpu.make_async_copy(part_out.at[dest], got_out.at[me], part_sem).start()
                pltpu.make_async_copy(part_ml.at[g], got_ml.at[me], ml_sem).start()

    pltpu.make_async_copy(got_ml, got_ml, ml_sem).wait()
    peaks = got_ml[:, 0, :]
    scale = jnp.exp2((peaks - jnp.max(peaks, axis=0, keepdims=True)) * factor)
    whole = jnp.sum(scale * got_ml[:, 1, :], axis=0, keepdims=True)
    scale = scale / whole
    pltpu.make_async_copy(got_out, got_out, part_sem).wait()
    merged = jnp.zeros((share, HD), jnp.float32)
    for s in range(n):
        merged = merged + got_out[s].astype(jnp.float32) * scale[s : s + 1, :]
    piece[...] = merged.astype(jnp.bfloat16)

    @pl.loop(1, n // 2)
    def _(i):
        pltpu.make_async_remote_copy(
            src_ref=piece,
            dst_ref=pieces.at[core, chip],
            send_sem=send_sem.at[5],
            recv_sem=piece_sem.at[mine],
            device_id=(lax.rem(me + 2 * i, n),),
            device_id_type=MESH,
        ).start()

    pltpu.make_async_copy(piece, pieces.at[core, chip], piece_sem.at[mine]).start()

    hand_on(pieces, order[0], piece_sem, piece_pair_sem, send_sem.at[7])
    for t, g in enumerate(order):
        if t + 1 < KVH:
            hand_on(pieces, order[t + 1], piece_sem, piece_pair_sem, send_sem.at[7])
        await_pair(pieces, g, piece_pair_sem)
        tall = jnp.concatenate(
            [pieces[j % 2, g * half + j // 2].astype(jnp.float32) for j in range(per)], axis=0
        )
        flat = jnp.transpose(tall).astype(jnp.bfloat16)
        for i in range(group):
            start = pl.multiple_of((g * group + i) * HD, HD)
            out_ref[:, pl.ds(start, HD)] = flat[i * rows : (i + 1) * rows]

    others, chips = pl.ds(0, n - 1), pl.ds(0, n // 2 - 1)
    for i, ref in (
        (0, q_all.at[0, chips]),
        (3, got_out.at[others]),
        (4, got_ml.at[others]),
        (5, pieces.at[0, chips]),
        (6, q_all.at[0]),
        (7, pieces.at[0]),
    ):
        pltpu.make_async_copy(ref, ref, send_sem.at[i]).wait()

    @pl.when(me != 0)
    def _():
        pltpu.make_async_copy(k_own, k_own, send_sem.at[1]).wait()
        pltpu.make_async_copy(v_own, v_own, send_sem.at[2]).wait()


def solution(mesh):
    n = mesh.shape["seq"]

    def per_device(q, k, v, positions, span_segments, cache_keys, cache_values, cache_segments):
        rows, width = q.shape
        kwidth = k.shape[1]
        tokens = cache_keys.shape[0]
        share = KVH * HD // n
        bf16, f32, i32 = jnp.bfloat16, jnp.float32, jnp.int32
        return pl.pallas_call(
            functools.partial(kernel, n),
            out_shape=jax.ShapeDtypeStruct((rows, H * HD), bf16),
            in_specs=[pl.BlockSpec(memory_space=pl.ANY)] * 8,
            out_specs=pl.BlockSpec(memory_space=pltpu.VMEM),
            scratch_shapes=[
                pltpu.VMEM((rows, width), bf16),
                pltpu.VMEM((rows, kwidth), bf16),
                pltpu.VMEM((rows, kwidth), bf16),
                pltpu.SMEM(positions.shape, i32),
                pltpu.SMEM(span_segments.shape, i32),
                pltpu.VMEM((tokens, KVH * HD), bf16),
                pltpu.VMEM((tokens, KVH * HD), bf16),
                pltpu.VMEM((1, tokens), i32),
                pltpu.VMEM((2, n // 2, rows, width), bf16),
                pltpu.VMEM((n, rows, kwidth), bf16),
                pltpu.VMEM((n, rows, kwidth), bf16),
                pltpu.VMEM((rows, KVH * HD), bf16),
                pltpu.VMEM((rows, KVH * HD), bf16),
                pltpu.VMEM((KVH, HD, tokens), bf16),
                pltpu.VMEM((tokens, HD), f32),
                pltpu.VMEM((n, share, HD), bf16),
                pltpu.VMEM((KVH, 2, HD), f32),
                pltpu.VMEM((n, share, HD), bf16),
                pltpu.VMEM((n, 2, HD), f32),
                pltpu.VMEM((share, HD), bf16),
                pltpu.VMEM((2, n // 2, share, HD), bf16),
                pltpu.SemaphoreType.DMA((8,)),
                pltpu.SemaphoreType.DMA((KVH,)),
                pltpu.SemaphoreType.DMA((KVH,)),
                pltpu.SemaphoreType.DMA((2,)),
                pltpu.SemaphoreType.DMA,
                pltpu.SemaphoreType.DMA,
                pltpu.SemaphoreType.DMA((KVH,)),
                pltpu.SemaphoreType.DMA((KVH,)),
                pltpu.SemaphoreType.DMA((8,)),
            ],
            compiler_params=pltpu.CompilerParams(collective_id=0, has_side_effects=True),
        )(
            q,
            k,
            v,
            positions,
            span_segments,
            cache_keys,
            cache_values,
            cache_segments.reshape(1, tokens),
        )

    in_specs = (
        P(None, "seq"),
        P(None, "seq"),
        P(None, "seq"),
        P(),
        P(),
        P("seq", None),
        P("seq", None),
        P("seq"),
    )
    return jax.shard_map(
        per_device, mesh=mesh, in_specs=in_specs, out_specs=P(), check_vma=False
    )
```

```python
import functools
import math

import jax
import jax.numpy as jnp
import numpy as np
from jax import lax
from jax.experimental import pallas as pl
from jax.experimental.pallas import tpu as pltpu
from jax.sharding import PartitionSpec as P

H = 64
KVH = 8
HD = 128
MESH = pl.DeviceIdType.MESH
HIDDEN = -1e30
FLOOR = -1e29


def rope_tables(pos, rows):
    half = HD // 2
    lane = lax.broadcasted_iota(jnp.int32, (rows, HD), 1)
    row = lax.broadcasted_iota(jnp.int32, (rows, HD), 0)
    index = lax.rem(lane, half)
    inverse = jnp.zeros((rows, HD), jnp.float32)
    for j in range(half):
        inverse = jnp.where(index == j, jnp.float32(np.float32(1e6 ** (-2.0 * j / HD))), inverse)
    chosen = []
    for c in range(3):
        spread = jnp.zeros((rows, HD), jnp.int32)
        for r in range(rows):
            spread = jnp.where(row == r, pos[c, r], spread)
        chosen.append(spread)
    picked = jnp.where(
        index < HD // 8, chosen[0], jnp.where(index < 5 * HD // 16, chosen[1], chosen[2])
    )
    angle = picked.astype(jnp.float32) * inverse
    sine = jnp.sin(angle)
    return jnp.cos(angle), jnp.where(lane < half, -sine, sine)


def columns(buf, start, width):
    if width >= HD:
        slot, off = start // width, start % width
        return buf[slot, :, off : off + HD].astype(jnp.float32)
    first = start // width
    return jnp.concatenate(
        [buf[first + i].astype(jnp.float32) for i in range(HD // width)], axis=1
    )


def group_head(buf, g, head):
    width = buf.shape[3]
    base = g * (buf.shape[1] // KVH)
    if width >= HD:
        block, off = head * HD // width, head * HD % width
        return buf[block % 2, base + block // 2, :, off : off + HD].astype(jnp.float32)
    first = head * (HD // width)
    return jnp.concatenate(
        [
            buf[block % 2, base + block // 2].astype(jnp.float32)
            for block in range(first, first + HD // width)
        ],
        axis=1,
    )


def kernel(
    n,
    q_hbm,
    k_hbm,
    v_hbm,
    pos_hbm,
    seg_hbm,
    ck_hbm,
    cv_hbm,
    cs_hbm,
    out_ref,
    q_own,
    k_own,
    v_own,
    pos,
    seg,
    keys,
    values,
    cseg,
    q_all,
    k_all,
    v_all,
    k_span,
    v_span,
    values_t,
    bias,
    part_out,
    part_ml,
    got_out,
    got_ml,
    piece,
    pieces,
    load_sem,
    q_sem,
    kv_sem,
    part_sem,
    ml_sem,
    piece_sem,
    send_sem,
):
    me = lax.axis_index("seq")
    rows, width = q_own.shape
    kwidth = k_own.shape[1]
    tokens = keys.shape[0]
    per = n // KVH
    share = HD // per
    mine = me // per
    half = per // 2
    core, chip = lax.rem(me, 2), me // 2

    def await_group(buf, g, sem):
        landed = buf.at[:, pl.ds(g * half, half)]
        pltpu.make_async_copy(landed, landed, sem.at[g]).wait()

    order = [lax.rem(mine + t, KVH) for t in range(KVH)]

    loads = [
        pltpu.make_async_copy(src, dst, load_sem.at[i])
        for i, (src, dst) in enumerate(
            (
                (q_hbm, q_own),
                (k_hbm, k_own),
                (v_hbm, v_own),
                (pos_hbm, pos),
                (seg_hbm, seg),
                (cs_hbm, cseg),
                (cv_hbm, values),
                (ck_hbm, keys),
            )
        )
    ]
    for load in loads:
        load.start()

    barrier = pltpu.get_barrier_semaphore()

    @pl.loop(1, n)
    def _(i):
        pl.semaphore_signal(
            barrier, inc=1, device_id=(lax.rem(me + i, n),), device_id_type=MESH
        )

    for load in loads[:3]:
        load.wait()
    own_q = pltpu.make_async_copy(q_own, q_all.at[core, chip], q_sem.at[mine])
    own_q.start()
    pl.semaphore_wait(barrier, n - 1)

    @pl.when(me != 0)
    def _():
        for i, (src, dst) in enumerate(((k_own, k_all), (v_own, v_all))):
            pltpu.make_async_remote_copy(
                src_ref=src,
                dst_ref=dst.at[me],
                send_sem=send_sem.at[1 + i],
                recv_sem=kv_sem.at[i],
                device_id=(0,),
                device_id_type=MESH,
            ).start()

    @pl.when(me == 0)
    def _():
        for i, (src, dst) in enumerate(((k_own, k_all), (v_own, v_all))):
            pltpu.make_async_copy(src, dst.at[me], kv_sem.at[i]).start()

    @pl.loop(1, n)
    def _(i):
        pltpu.make_async_remote_copy(
            src_ref=q_own,
            dst_ref=q_all.at[core, chip],
            send_sem=send_sem.at[0],
            recv_sem=q_sem.at[mine],
            device_id=(lax.rem(me + i, n),),
            device_id_type=MESH,
        ).start()

    for load in loads[3:]:
        load.wait()
    cosine, sine = rope_tables(pos, rows)
    lane = lax.broadcasted_iota(jnp.int32, (1, HD), 1)
    lane_row = lax.rem(lane, rows)
    lane_seg = jnp.zeros((1, HD), jnp.int32)
    for r in range(rows):
        lane_seg = jnp.where(lane_row == r, seg[r], lane_seg)
    lane_seg = lane_seg.astype(jnp.float32)
    for c in range(tokens // HD):
        across = cseg[:, c * HD : (c + 1) * HD].astype(jnp.float32)
        down = jnp.transpose(jnp.broadcast_to(across, (HD, HD)))
        bias[c * HD : (c + 1) * HD, :] = jnp.where(down == lane_seg, 0.0, HIDDEN)
    token = lax.broadcasted_iota(jnp.int32, (rows, HD), 0)
    token_seg = jnp.zeros((rows, HD), jnp.int32)
    for r in range(rows):
        token_seg = jnp.where(token == r, seg[r], token_seg)
    seen = (token_seg.astype(jnp.float32) == lane_seg) & (token <= lane_row)
    holder = jnp.where(me == 0, 0.0, HIDDEN)
    span_bias = jnp.where(seen, holder, HIDDEN)
    for g in range(KVH):
        values_t[g] = jnp.transpose(values[:, g * HD : (g + 1) * HD])

    @pl.when(me == 0)
    def _():
        for i, dst in enumerate((k_all, v_all)):
            pltpu.make_async_copy(dst, dst, kv_sem.at[i]).wait()
        for g in range(KVH):
            cols = slice(g * HD, (g + 1) * HD)
            k = columns(k_all, g * HD, kwidth)
            k_span[:, cols] = (k * cosine + pltpu.roll(k, HD // 2, 1) * sine).astype(jnp.bfloat16)
            v_span[:, cols] = columns(v_all, g * HD, kwidth).astype(jnp.bfloat16)

    @pl.when(me != 0)
    def _():
        k_span[...] = jnp.zeros_like(k_span)
        v_span[...] = jnp.zeros_like(v_span)

    contract_last = (((1,), (1,)), ((), ()))
    contract_first = (((0,), (0,)), ((), ()))
    factor = math.log2(math.e) / math.sqrt(HD)
    group = H // KVH
    for g in order:
        cols = pl.ds(pl.multiple_of(g * HD, HD), HD)
        await_group(q_all, g, q_sem)
        heads = []
        for i in range(group):
            q = group_head(q_all, g, i)
            heads.append((q * cosine + pltpu.roll(q, HD // 2, 1) * sine).astype(jnp.bfloat16))
        block = jnp.concatenate(heads, axis=0)
        scores = (
            lax.dot_general(keys[:, cols], block, contract_last, preferred_element_type=jnp.float32)
            + bias[...]
        )
        span_scores = (
            lax.dot_general(
                k_span[:, cols], block, contract_last, preferred_element_type=jnp.float32
            )
            + span_bias
        )
        peak = jnp.maximum(
            jnp.max(scores, axis=0, keepdims=True), jnp.max(span_scores, axis=0, keepdims=True)
        )
        peak = jnp.maximum(peak, FLOOR)
        weights = jnp.exp2((scores - peak) * factor)
        span_weights = jnp.exp2((span_scores - peak) * factor)
        total = jnp.sum(weights, axis=0, keepdims=True) + jnp.sum(
            span_weights, axis=0, keepdims=True
        )
        out = jnp.dot(
            values_t[g], weights.astype(jnp.bfloat16), preferred_element_type=jnp.float32
        ) + lax.dot_general(
            v_span[:, cols],
            span_weights.astype(jnp.bfloat16),
            contract_first,
            preferred_element_type=jnp.float32,
        )
        part_ml[g] = jnp.concatenate([peak, total], axis=0)
        for j in range(per):
            part_out[g * per + j] = out[j * share : (j + 1) * share].astype(jnp.bfloat16)

        @pl.loop(0, per)
        def _(j):
            dest = g * per + j

            @pl.when(dest != me)
            def _():
                pltpu.make_async_remote_copy(
                    src_ref=part_out.at[dest],
                    dst_ref=got_out.at[me],
                    send_sem=send_sem.at[3],
                    recv_sem=part_sem,
                    device_id=(dest,),
                    device_id_type=MESH,
                ).start()
                pltpu.make_async_remote_copy(
                    src_ref=part_ml.at[g],
                    dst_ref=got_ml.at[me],
                    send_sem=send_sem.at[4],
                    recv_sem=ml_sem,
                    device_id=(dest,),
                    device_id_type=MESH,
                ).start()

            @pl.when(dest == me)
            def _():
                pltpu.make_async_copy(part_out.at[dest], got_out.at[me], part_sem).start()
                pltpu.make_async_copy(part_ml.at[g], got_ml.at[me], ml_sem).start()

    pltpu.make_async_copy(got_ml, got_ml, ml_sem).wait()
    peaks = got_ml[:, 0, :]
    scale = jnp.exp2((peaks - jnp.max(peaks, axis=0, keepdims=True)) * factor)
    whole = jnp.sum(scale * got_ml[:, 1, :], axis=0, keepdims=True)
    scale = scale / whole
    pltpu.make_async_copy(got_out, got_out, part_sem).wait()
    merged = jnp.zeros((share, HD), jnp.float32)
    for s in range(n):
        merged = merged + got_out[s].astype(jnp.float32) * scale[s : s + 1, :]
    piece[...] = merged.astype(jnp.bfloat16)

    @pl.loop(1, n)
    def _(i):
        pltpu.make_async_remote_copy(
            src_ref=piece,
            dst_ref=pieces.at[core, chip],
            send_sem=send_sem.at[5],
            recv_sem=piece_sem.at[mine],
            device_id=(lax.rem(me + i, n),),
            device_id_type=MESH,
        ).start()

    pltpu.make_async_copy(piece, pieces.at[core, chip], piece_sem.at[mine]).start()

    for g in order:
        await_group(pieces, g, piece_sem)
        tall = jnp.concatenate(
            [pieces[j % 2, g * half + j // 2].astype(jnp.float32) for j in range(per)], axis=0
        )
        flat = jnp.transpose(tall).astype(jnp.bfloat16)
        for i in range(group):
            start = pl.multiple_of((g * group + i) * HD, HD)
            out_ref[:, pl.ds(start, HD)] = flat[i * rows : (i + 1) * rows]

    others, chips = pl.ds(0, n - 1), pl.ds(0, n // 2 - 1)
    for i, ref in (
        (0, q_all.at[0, chips]),
        (3, got_out.at[others]),
        (4, got_ml.at[others]),
        (5, pieces.at[0, chips]),
        (0, q_all.at[1]),
        (5, pieces.at[1]),
    ):
        pltpu.make_async_copy(ref, ref, send_sem.at[i]).wait()

    @pl.when(me != 0)
    def _():
        pltpu.make_async_copy(k_own, k_own, send_sem.at[1]).wait()
        pltpu.make_async_copy(v_own, v_own, send_sem.at[2]).wait()


def solution(mesh):
    n = mesh.shape["seq"]

    def per_device(q, k, v, positions, span_segments, cache_keys, cache_values, cache_segments):
        rows, width = q.shape
        kwidth = k.shape[1]
        tokens = cache_keys.shape[0]
        share = KVH * HD // n
        bf16, f32, i32 = jnp.bfloat16, jnp.float32, jnp.int32
        return pl.pallas_call(
            functools.partial(kernel, n),
            out_shape=jax.ShapeDtypeStruct((rows, H * HD), bf16),
            in_specs=[pl.BlockSpec(memory_space=pl.ANY)] * 8,
            out_specs=pl.BlockSpec(memory_space=pltpu.VMEM),
            scratch_shapes=[
                pltpu.VMEM((rows, width), bf16),
                pltpu.VMEM((rows, kwidth), bf16),
                pltpu.VMEM((rows, kwidth), bf16),
                pltpu.SMEM(positions.shape, i32),
                pltpu.SMEM(span_segments.shape, i32),
                pltpu.VMEM((tokens, KVH * HD), bf16),
                pltpu.VMEM((tokens, KVH * HD), bf16),
                pltpu.VMEM((1, tokens), i32),
                pltpu.VMEM((2, n // 2, rows, width), bf16),
                pltpu.VMEM((n, rows, kwidth), bf16),
                pltpu.VMEM((n, rows, kwidth), bf16),
                pltpu.VMEM((rows, KVH * HD), bf16),
                pltpu.VMEM((rows, KVH * HD), bf16),
                pltpu.VMEM((KVH, HD, tokens), bf16),
                pltpu.VMEM((tokens, HD), f32),
                pltpu.VMEM((n, share, HD), bf16),
                pltpu.VMEM((KVH, 2, HD), f32),
                pltpu.VMEM((n, share, HD), bf16),
                pltpu.VMEM((n, 2, HD), f32),
                pltpu.VMEM((share, HD), bf16),
                pltpu.VMEM((2, n // 2, share, HD), bf16),
                pltpu.SemaphoreType.DMA((8,)),
                pltpu.SemaphoreType.DMA((KVH,)),
                pltpu.SemaphoreType.DMA((2,)),
                pltpu.SemaphoreType.DMA,
                pltpu.SemaphoreType.DMA,
                pltpu.SemaphoreType.DMA((KVH,)),
                pltpu.SemaphoreType.DMA((6,)),
            ],
            compiler_params=pltpu.CompilerParams(collective_id=0, has_side_effects=True),
        )(
            q,
            k,
            v,
            positions,
            span_segments,
            cache_keys,
            cache_values,
            cache_segments.reshape(1, tokens),
        )

    in_specs = (
        P(None, "seq"),
        P(None, "seq"),
        P(None, "seq"),
        P(),
        P(),
        P("seq", None),
        P("seq", None),
        P("seq"),
    )
    return jax.shard_map(
        per_device, mesh=mesh, in_specs=in_specs, out_specs=P(), check_vma=False
    )
```
